128 devices in a mesh: walk: 8 (over y, z_hi), chol: 16 (over z_lo, x, core).
Axes of the slice: x: 4, y: 4, z: 4 (z_hi: 2, z_lo: 2; z = z_hi * 2 + z_lo), core: 2. Of those that a mesh axis runs over, the one named last changes fastest.
Arguments:
- orbitals: bfloat16 [1024, 64, 1024], P(('walk', 'chol')), may hold values from -6 to 6
- cholesky: bfloat16 [192, 64, 1024], P('chol'), may hold values from -0.1875 to 0.1875
- parents: int32 [1024], P(('walk', 'chol')), may hold values from 0 to 1023, as said below
- counts: int32 [8, 16], P('walk', 'chol'), may hold values from 1 to 8, as said below
- steps: bfloat16 [1024, 64, 1024], P(('walk', 'chol')), may hold values from -6 to 6
Outputs:
- energy: float32 [1024], P(('walk', 'chol'))
- parent_grad: float32 [1024, 64, 1024], P(('walk', 'chol'))
The draws below stay inside these ranges and needn't reach their ends.
Inputs may be any that keep to these rules, and one draw needn't show every extreme that they name: The parent of a new walker lies on the same index of chol as the walker. Of one device's new walkers at most 2 have parents on any one index of walk, and on some index exactly 2. The first counts entries of a device's 8 new walkers are live; in every draw some device is full.
All inputs are finite; a program needn't handle non-finite values.
Results may differ from the reference program's by a relative error of at most 0.0044.
Values may be sent and summed in bfloat16 or wider, within the bound.
A program may use at most 128 MiB of HBM per device.

```python
import jax
import jax.numpy as jnp
from jax import lax

BASIS = 1024
ELECTRONS = 64
WALK_DEV = 8
CHOL_DEV = 12
WALKERS = 1024
VECTORS = 192
N_WALK = 8
N_CHOL = 16


def draw_parents(key, part):
    devices_all = N_WALK * N_CHOL
    first, second, third, fourth = jax.random.split(jax.random.fold_in(key, 11), 4)
    walk_orders = jax.vmap(lambda sub: jax.random.permutation(sub, N_WALK))(jax.random.split(first, devices_all))
    allow = 1 if WALK_DEV // 2 < N_WALK else 0
    offset = jax.random.randint(second, (devices_all, 1), 0, 2) * allow
    within = jnp.arange(WALK_DEV, dtype=jnp.int32)[None, :]
    choice_index = jnp.where(within < 2, 0, (within + offset) // 2)
    shuffles = jax.vmap(lambda sub: jax.random.permutation(sub, WALK_DEV))(jax.random.split(third, devices_all))
    choice_index = jnp.take_along_axis(choice_index, shuffles, axis=1)
    source_walk = jnp.take_along_axis(walk_orders, choice_index, axis=1)
    source_slot = jax.random.randint(fourth, (devices_all, WALK_DEV), 0, WALK_DEV)
    chol_index = (jnp.arange(devices_all, dtype=jnp.int32) % N_CHOL)[:, None]
    parent_ids = (source_walk * N_CHOL + chol_index) * WALK_DEV + source_slot
    return parent_ids.reshape(-1).astype(jnp.int32)


def draw_counts(key, part):
    first, second = jax.random.split(jax.random.fold_in(key, 23), 2)
    lowered = jax.random.randint(first, (N_WALK * N_CHOL,), 0, WALK_DEV)
    lowered = lowered * jax.random.randint(second, (N_WALK * N_CHOL,), 0, 2)
    filled = jnp.maximum(WALK_DEV - lowered, 1)
    pick = jax.random.randint(jax.random.fold_in(key, 29), (), 0, N_WALK * N_CHOL)
    filled = jnp.where(jnp.arange(N_WALK * N_CHOL) == pick, WALK_DEV, filled)
    return filled.reshape(N_WALK, N_CHOL).astype(jnp.int32)


def block_levels(own_key, extent, cuts, smallest, high):
    factor_of, own = 1.0, jax.random.fold_in(own_key, 6)
    for dim, blocks in cuts:
        steps = jnp.exp(jax.random.uniform(jax.random.fold_in(own, dim), (blocks,), jnp.float32, smallest / len(cuts), high / len(cuts)))
        factor_of = factor_of * jnp.repeat(steps, extent[dim] // blocks).reshape([-1 if axis == dim else 1 for axis in range(len(extent))])
    return factor_of


def normal_values(key, extent, width, most, cuts=(), held_as=jnp.bfloat16):
    values = width * jax.random.normal(key, extent, jnp.float32)
    if cuts:
        values = values * block_levels(key, extent, cuts, -0.22, 0.18)
    return jnp.clip(values, -most, most).astype(held_as)


def setup_inputs(seed: int = 0) -> dict:
    splits = jax.random.split(jax.random.key(seed), 6)
    orbitals = normal_values(splits[0], (WALKERS, ELECTRONS, BASIS), 1.0, 6.0, ((0, 128),))
    cholesky = normal_values(splits[1], (VECTORS, ELECTRONS, BASIS), BASIS ** -0.5, 0.1875, ((0, 16),))
    parents = draw_parents(jax.random.fold_in(splits[5], 71), 0)
    counts = draw_counts(jax.random.fold_in(splits[5], 71), 0)
    steps = normal_values(splits[4], (WALKERS, ELECTRONS, BASIS), 1.0, 6.0, ((0, 128),))
    return dict(orbitals=orbitals, cholesky=cholesky, parents=parents, counts=counts, steps=steps)


def reference(orbitals, cholesky, parents, counts, steps):
    clones = (orbitals[parents].astype(jnp.float32) + steps.astype(jnp.float32)).astype(jnp.bfloat16)
    position = jnp.arange(WALKERS, dtype=jnp.int32)
    flat_counts = counts.reshape(-1)
    alive = (position % WALK_DEV < flat_counts[position // WALK_DEV]).astype(jnp.float32)
    blocks = clones.reshape(N_WALK, WALK_DEV * N_CHOL, ELECTRONS, BASIS)

    def shard_step(total, shard):
        vectors = lax.dynamic_slice_in_dim(cholesky, (shard * CHOL_DEV).astype(jnp.int32), CHOL_DEV, 0).astype(jnp.float32)

        def one_block(walkers):
            walk_f = walkers.astype(jnp.float32)
            intersection = jnp.einsum("gip,wjp->wgij", vectors, walk_f).astype(jnp.bfloat16).astype(jnp.float32)
            part = -jnp.einsum("wgji,gip->wjp", intersection, vectors)
            part = lax.optimization_barrier(part.astype(jnp.bfloat16))
            return part.astype(jnp.float32)

        parts = lax.map(one_block, blocks).reshape(WALKERS, ELECTRONS, BASIS)
        return total + parts, None

    start = jnp.zeros((WALKERS, ELECTRONS, BASIS), jnp.float32)
    summed, _ = lax.scan(shard_step, start, jnp.arange(N_CHOL, dtype=jnp.int32))
    gradient = summed * alive[:, None, None]
    energy = 0.5 * jnp.sum(clones.astype(jnp.float32) * gradient, axis=(1, 2))
    parent_grad = jax.ops.segment_sum(gradient, parents, num_segments=WALKERS)
    return energy, parent_grad
```

```python
import functools

import jax
import jax.numpy as jnp
from jax import lax
from jax.experimental import pallas as pl
from jax.experimental.pallas import tpu as pltpu
from jax.sharding import Mesh
from jax.sharding import PartitionSpec as P

NAMES = ("y", "h", "l", "x", "k")
MESH = pl.DeviceIdType.MESH
CAP = 2
NY, NH, NX = 4, 2, 4
CHUNKS = 4
EARLY = 4

ORDER = ("H0", "H1", "X00", "X01", "X02", "P0", "X03", "X10", "O0", "X11", "O1", "O3", "O2", "P1", "X12", "X13")
BLOCK = {name: i for i, name in enumerate(ORDER)}


def pair_piece(i, dk):
    return (BLOCK[f"P{i // 2}"], (i % 2) * 2 + dk)


def x_piece(dz, side, i, dk):
    return (BLOCK[f"X{dz}{i}"], side + 2 * dk)


def far_piece(dz, r, dk):
    return (BLOCK[f"O{r}"], dz + 2 * dk)


def piece_id(piece):
    return piece[0] * CHUNKS + piece[1]


class Links:
    def __init__(self, store, send_sem, recv_sem, peers, depth):
        self.store, self.send_sem, self.recv_sem = store, send_sem, recv_sem
        self.peers, self.depth = peers, depth
        self.sends = {}

    def view(self, piece):
        return self.store.at[piece[0], pl.ds(piece[1] * self.depth, self.depth)]

    def send(self, source, piece, peer, key=None):
        copy = pltpu.make_async_remote_copy(
            src_ref=source,
            dst_ref=self.view(piece),
            send_sem=self.send_sem.at[self.sends.setdefault((piece, key or peer), len(self.sends))],
            recv_sem=self.recv_sem.at[piece_id(piece)],
            device_id=self.peers[peer],
            device_id_type=MESH,
        )
        copy.start()

    def forward(self, piece, target, peer, key=None):
        self.send(self.view(piece), target, peer, key)

    def any_copy(self, piece, send_sem, recv_sem):
        here = self.view(piece)
        return pltpu.make_async_remote_copy(
            src_ref=here,
            dst_ref=here,
            send_sem=send_sem,
            recv_sem=recv_sem,
            device_id=self.peers["core"],
            device_id_type=MESH,
        )

    def wait(self, piece):
        self.any_copy(piece, self.send_sem.at[0], self.recv_sem.at[piece_id(piece)]).wait_recv()

    def finish(self):
        for n in range(len(self.sends)):
            self.any_copy((0, 0), self.send_sem.at[n], self.recv_sem.at[0]).wait_send()


def half_step(store, turned, inter, total, t):
    electrons, basis = store.shape[2:]
    early, late = t < EARLY, t < 2 * EARLY
    g = jnp.where(late, jnp.where(early, 0, 1), lax.rem(t, 2))
    b = jnp.where(late, jnp.where(early, t, t - EARLY), t // 2)
    block = store.at[b]
    for n in range(turned.shape[2] // 256):
        for m in range(store.shape[1] // 4):
            vectors = block[4 * m : 4 * m + 4].reshape(4 * electrons, basis)
            made = jnp.dot(vectors, turned[g, :, n * 256 : (n + 1) * 256], preferred_element_type=jnp.float32)
            made = made.astype(jnp.bfloat16)
            for v in range(0, 4, 2):
                for s in range(0, 4, 2):
                    a = made[v * 64 : v * 64 + 64, s * 64 : s * 64 + 128]
                    c = made[v * 64 + 64 : v * 64 + 128, s * 64 : s * 64 + 128]
                    row, col = (4 * n + s) * 64, (4 * m + v) * 64
                    inter[row : row + 64, col : col + 128] = jnp.concatenate([a[:, :64], c[:, :64]], axis=1)
                    inter[row + 64 : row + 128, col : col + 128] = jnp.concatenate([a[:, 64:], c[:, 64:]], axis=1)
    for n in range(basis // 256):
        part = block[:, :, n * 256 : (n + 1) * 256].reshape(-1, 256)
        total[g, :, n * 256 : (n + 1) * 256] += jnp.dot(inter[...], part, preferred_element_type=jnp.float32)


def kernel(
    parents, counts, orbitals_hbm, cholesky_hbm, steps_hbm, energy_ref, grad_ref,
    store, orb, stp, out, slots, tag_out, tags, turned, total, inter, weights, e_out, e_in,
    load_sem, slot_send, slot_recv, tag_send, tag_recv, e_send, e_recv, piece_send, piece_recv,
):
    y, h, l, x, k = (lax.axis_index(name) for name in NAMES)
    per_device, electrons, basis = orb.shape
    depth = store.shape[1] // CHUNKS
    half = NY * CAP * electrons

    loads = [
        pltpu.make_async_copy(src, dst, load_sem.at[i])
        for i, (src, dst) in enumerate(((steps_hbm, stp), (cholesky_hbm, store.at[0]), (orbitals_hbm, orb)))
    ]
    for load in loads:
        load.start()

    up, down = {"x": lax.rem(x + 1, NX)}, {"x": lax.rem(x + NX - 1, NX)}
    peers = {
        "x+": up,
        "x-": down,
        "pair": {"l": 1 - l},
        "core": {"k": 1 - k},
        "y+": {"y": lax.rem(y + 1, NY)},
        "y-": {"y": lax.rem(y + NY - 1, NY)},
    }
    walk_ids = [(dh, dy) for dh in range(NH) for dy in (1, 3, 2, 0) if (dh, dy) != (0, 0)]
    walk_to = {(dh, dy): {"y": lax.rem(y + dy, NY), "h": lax.rem(h + dh, NH)} for dh, dy in walk_ids}
    walk_from = {(dh, dy): {"y": lax.rem(y + NY - dy, NY), "h": lax.rem(h + dh, NH)} for dh, dy in walk_ids}

    barrier = pltpu.get_barrier_semaphore()
    greeted = list(walk_to.values()) + [peers[p] for p in ("x+", "x-", "pair", "core")]
    for peer in greeted:
        pl.semaphore_signal(barrier, inc=1, device_id=peer, device_id_type=MESH)

    chol_walkers = 16 * per_device
    parent = [parents[0, j] for j in range(per_device)]
    owner = [p // chol_walkers for p in parent]
    keys = []
    for j in range(per_device):
        rank = sum([jnp.where(owner[i] == owner[j], 1, 0) for i in range(j)], jnp.int32(0))
        keys.append(owner[j] * CAP + rank)
    rows = lax.broadcasted_iota(jnp.int32, (per_device, 128), 0)
    loads[0].wait()
    walker_of, live_of = {}, {}
    for dh in range(NH):
        for dy in range(NY):
            device = lax.rem(y + dy, NY) * NH + lax.rem(h + dh, NH)
            for r in range(CAP):
                key = device * CAP + r
                index, mark, live = jnp.int32(0), jnp.int32(-1), jnp.int32(0)
                for j in range(per_device):
                    hit = keys[j] == key
                    alive = jnp.logical_and(hit, j < counts[0, 0])
                    index = jnp.where(hit, j, index)
                    mark = jnp.where(alive, parent[j] % per_device, mark)
                    live = jnp.where(alive, 1, live)
                walker_of[dh, dy, r], live_of[dh, dy, r] = index, live
                tag = jnp.where(rows == mark, 1.0, 0.0).astype(jnp.float32)
                if (dh, dy) == (0, 0):
                    slots[0, 0, r] = stp[index]
                    tags[0, 0, r] = tag
                else:
                    out[dh, dy, r] = stp[index]
                    tag_out[dh, dy, r] = tag
    loads[1].wait()
    pl.semaphore_wait(barrier, len(greeted))

    def remote(source, target, send, recv, peer):
        return pltpu.make_async_remote_copy(
            src_ref=source, dst_ref=target, send_sem=send, recv_sem=recv, device_id=peer, device_id_type=MESH
        )

    tag_copies, slot_copies = {}, {}
    for dh, dy in walk_ids:
        n, at = dh * NY + dy, (dh, dy)
        tag_copies[at] = remote(tag_out.at[at], tags.at[at], tag_send.at[n], tag_recv.at[n], walk_to[at])
        slot_copies[at] = remote(out.at[at], slots.at[at], slot_send.at[n], slot_recv.at[n], walk_to[at])
        tag_copies[at].start()
        slot_copies[at].start()

    links = Links(store, piece_send, piece_recv, peers, depth)

    def own(i):
        return store.at[0, pl.ds(lax.rem(y + i, CHUNKS) * depth, depth)]

    for i in range(CHUNKS):
        links.send(own(i), (BLOCK["H1"], i), "core")
        if i < 2:
            links.send(own(i), x_piece(0, 0, i, 0), "x+")
            links.send(own(i), x_piece(0, 1, i, 0), "x-")
    for i in range(2):
        links.send(own(i), pair_piece(i, 0), "pair")

    def x_arrived(dz, i):
        for side in range(2):
            piece = x_piece(dz, side, i, 0)
            links.wait(piece)
            links.forward(piece, x_piece(dz, side, i, 1), "core")

    def first_x():
        x_arrived(0, 0)

        @pl.when(k == 0)
        def _():
            links.forward(x_piece(0, 0, 0, 0), far_piece(0, 0, 0), "x+", "x")

        @pl.when(k == 1)
        def _():
            links.forward(x_piece(0, 1, 0, 0), far_piece(0, 0, 0), "x-", "x")

        for i in (2, 3):
            links.send(own(i), x_piece(0, 0, i, 0), "x+")
            links.send(own(i), x_piece(0, 1, i, 0), "x-")

    def pair_arrived(i):
        piece = pair_piece(i, 0)
        links.wait(piece)
        links.forward(piece, pair_piece(i, 1), "core")
        links.forward(piece, x_piece(1, 0, i, 0), "x+")
        links.forward(piece, x_piece(1, 1, i, 0), "x-")

    def far_arrived(dz):
        piece = far_piece(dz, 0, 0)
        links.wait(piece)
        links.forward(piece, far_piece(dz, 0, 1), "core")
        links.forward(piece, far_piece(dz, 3, 0), "y+")
        links.forward(piece, far_piece(dz, 1, 0), "y-")
        if dz == 0:
            links.forward(piece, far_piece(1, 0, 0), "pair")
            for i in (2, 3):
                links.send(own(i), pair_piece(i, 0), "pair")

    def far_turned(dz):
        for r, onward in ((3, "y+"), (1, "y-")):
            piece = far_piece(dz, r, 0)
            links.wait(piece)
            links.forward(piece, far_piece(dz, r, 1), "core")
            if (dz == 0) == (r == 3):
                links.forward(piece, far_piece(dz, 2, 0), onward)

    def far_last(dz):
        piece = far_piece(dz, 2, 0)
        links.wait(piece)
        links.forward(piece, far_piece(dz, 2, 1), "core")

    events = [
        (3, lambda: x_arrived(0, 1)),
        (6, lambda: far_arrived(0)),
        (7, lambda: pair_arrived(0)),
        (8, lambda: x_arrived(0, 2)),
        (9, lambda: pair_arrived(1)),
        (10, lambda: far_turned(0)),
        (12, lambda: x_arrived(0, 3)),
        (13, lambda: far_arrived(1)),
        (14, lambda: x_arrived(1, 0)),
        (15, lambda: pair_arrived(2)),
        (16, lambda: far_last(0)),
        (18, lambda: x_arrived(1, 1)),
        (19, lambda: pair_arrived(3)),
        (20, lambda: far_turned(1)),
        (22, lambda: far_last(1)),
        (26, lambda: x_arrived(1, 2)),
        (28, lambda: x_arrived(1, 3)),
    ]
    first_use = {}
    for place, name in enumerate(ORDER):
        first_use[name] = place if place < EARLY else 2 * place

    def clones(g):
        for dy in range(NY):
            if (g, dy) in slot_copies:
                tag_copies[g, dy].wait_recv()
                slot_copies[g, dy].wait_recv()

        def one_slot(s, carry):
            dy, r = s // CAP, s % CAP
            marks = [
                jnp.broadcast_to(tags[g, dy, r, i : i + 1, :], (16, 128)).astype(jnp.bfloat16) for i in range(per_device)
            ]
            for top in range(0, electrons, 16):
                for left in range(0, basis, 128):
                    found = jnp.zeros((16, 128), jnp.bfloat16)
                    for i in range(per_device):
                        found += orb[i, top : top + 16, left : left + 128] * marks[i]
                    step = slots[g, dy, r, top : top + 16, left : left + 128]
                    made = found.astype(jnp.float32) + step.astype(jnp.float32)
                    slots[g, dy, r, top : top + 16, left : left + 128] = made.astype(jnp.bfloat16)
            return carry

        lax.fori_loop(0, NY * CAP, one_slot, 0)
        turned[g] = slots[g].reshape(half, basis).T

    first_x()
    loads[2].wait()
    clones(0)
    total[...] = jnp.zeros_like(total)

    def with_events(t, carry):
        at = {}
        for when, event in events:
            at.setdefault(when, []).append(event)
        for name in ORDER[1:]:
            due = first_use[name]
            second = range(CHUNKS) if name == "H1" else (2, 3) if name[0] != "P" else (1, 3)
            pieces = [(BLOCK[name], m) for m in second]
            at.setdefault(due, []).append(lambda pieces=pieces: [links.wait(p) for p in pieces])
        for when in sorted(at):

            @pl.when(t == when)
            def _(when=when):
                for event in at[when]:
                    event()

        @pl.when(t == EARLY)
        def _():
            clones(1)

        half_step(store, turned, inter, total, t)
        return carry

    lax.fori_loop(0, 2 * len(ORDER), with_events, jnp.int32(0))

    def energy_of(s, carry):
        g, dy, r = s // (NY * CAP), s // CAP % NY, s % CAP
        base = pl.multiple_of((dy * CAP + r) * electrons, electrons)
        tile = jnp.zeros((8, 128), jnp.float32)
        for top in range(0, electrons, 16):
            for left in range(0, basis, 128):
                grad = total[g, pl.ds(base + top, 16), left : left + 128]
                made = slots[g, dy, r, top : top + 16, left : left + 128].astype(jnp.float32) * grad
                tile += made[:8] + made[8:]
        e_out[g, dy, r] = tile * -0.5
        return carry

    lax.fori_loop(0, NH * NY * CAP, energy_of, 0)
    e_copies = {}
    for dh, dy in walk_ids:
        n, at = dh * NY + dy, (dh, dy)
        e_copies[at] = remote(e_out.at[at], e_in.at[at], e_send.at[n], e_recv.at[n], walk_from[at])
        e_copies[at].start()

    for dh in range(NH):
        for dy in range(NY):
            for r in range(CAP):
                for i in range(per_device):
                    row = tags[dh, dy, r, i : i + 1, :]
                    weights[(dh * NY + dy) * CAP + r, i] = jnp.broadcast_to(-row, (8, 128))

    def gather(t, carry):
        top = pl.multiple_of(t // 8 * 8, 8)
        left = pl.multiple_of(t % 8 * 128, 128)
        sums = [jnp.zeros((8, 128), jnp.float32) for _ in range(per_device)]
        for s in range(NH * NY * CAP):
            g, at = s // (NY * CAP), s % (NY * CAP) * electrons
            grad = total[g, pl.ds(at + top, 8), pl.ds(left, 128)]
            for i in range(per_device):
                sums[i] += weights[s, i] * grad
        for i in range(per_device):
            grad_ref[i, pl.ds(top, 8), pl.ds(left, 128)] = sums[i]
        return carry

    lax.fori_loop(0, electrons * basis // 1024, gather, 0)

    for at in walk_ids:
        e_copies[at].wait()
    for j in range(per_device):
        tile = jnp.zeros((8, 128), jnp.float32)
        for dh in range(NH):
            for dy in range(NY):
                source = e_out if (dh, dy) == (0, 0) else e_in
                for r in range(CAP):
                    used = jnp.logical_and(walker_of[dh, dy, r] == j, live_of[dh, dy, r] == 1)
                    tile += jnp.where(used, 1.0, 0.0).astype(jnp.float32) * source[dh, dy, r]
        energy_ref[j] = tile

    for at in walk_ids:
        tag_copies[at].wait_send()
        slot_copies[at].wait_send()
    links.finish()


def body(orbitals, cholesky, parents, counts, steps):
    per_device, electrons, basis = orbitals.shape
    vectors = cholesky.shape[0]
    half = NY * CAP * electrons
    peers = (NH, NY)
    f32, bf16 = jnp.float32, jnp.bfloat16
    dma = pltpu.SemaphoreType.DMA
    energy, grad = pl.pallas_call(
        kernel,
        out_shape=(
            jax.ShapeDtypeStruct((per_device, 8, 128), f32),
            jax.ShapeDtypeStruct((per_device, electrons, basis), f32),
        ),
        in_specs=[pl.BlockSpec(memory_space=pltpu.SMEM)] * 2 + [pl.BlockSpec(memory_space=pl.ANY)] * 3,
        out_specs=(pl.BlockSpec(memory_space=pltpu.VMEM), pl.BlockSpec(memory_space=pltpu.VMEM)),
        scratch_shapes=[
            pltpu.VMEM((len(ORDER), vectors, electrons, basis), bf16),
            pltpu.VMEM((per_device, electrons, basis), bf16),
            pltpu.VMEM((per_device, electrons, basis), bf16),
            pltpu.VMEM((*peers, CAP, electrons, basis), bf16),
            pltpu.VMEM((*peers, CAP, electrons, basis), bf16),
            pltpu.VMEM((*peers, CAP, per_device, 128), f32),
            pltpu.VMEM((*peers, CAP, per_device, 128), f32),
            pltpu.VMEM((NH, basis, half), bf16),
            pltpu.VMEM((NH, half, basis), f32),
            pltpu.VMEM((half, vectors * electrons), bf16),
            pltpu.VMEM((NH * NY * CAP, per_device, 8, 128), f32),
            pltpu.VMEM((*peers, CAP, 8, 128), f32),
            pltpu.VMEM((*peers, CAP, 8, 128), f32),
            dma((3,)),
            *[dma((NH * NY,))] * 6,
            dma((64,)),
            dma((len(ORDER) * CHUNKS,)),
        ],
        compiler_params=pltpu.CompilerParams(
            collective_id=0, has_side_effects=True, vmem_limit_bytes=60 * 2**20
        ),
        name="exchange",
    )(parents.reshape(1, -1), counts, orbitals, cholesky, steps)
    return jnp.sum(energy, axis=(1, 2)), grad


def solution(mesh):
    torus = Mesh(mesh.devices.reshape(NY, NH, 2, NX, 2), NAMES)
    return jax.shard_map(
        body,
        mesh=torus,
        in_specs=(
            P(NAMES, None, None),
            P(("l", "x", "k"), None, None),
            P(NAMES),
            P(("y", "h"), ("l", "x", "k")),
            P(NAMES, None, None),
        ),
        out_specs=(P(NAMES), P(NAMES, None, None)),
        check_vma=False,
    )
```

```python
import functools

import jax
import jax.numpy as jnp
from jax import lax
from jax.experimental import pallas as pl
from jax.experimental.pallas import tpu as pltpu
from jax.sharding import Mesh
from jax.sharding import PartitionSpec as P

NAMES = ("y", "h", "l", "x", "k")
MESH = pl.DeviceIdType.MESH
CAP = 2
NY, NH, NX = 4, 2, 4
CHUNKS = 4
EARLY = 5

REACH = ((0, 0), (0, 1), (0, 3), (1, 0), (0, 2), (1, 1), (1, 3), (1, 2))

ORDER = ("H0", "H1", "X00", "X01", "X02", "X03", "P1", "P0", "X11", "O0", "X10", "X12", "O1", "X13", "O3", "O2")
BLOCK = {name: i for i, name in enumerate(ORDER)}


def pair_piece(i, dk):
    return (BLOCK[f"P{i // 2}"], (i % 2) * 2 + dk)


def x_piece(dz, side, i, dk):
    return (BLOCK[f"X{dz}{i}"], side + 2 * dk)


def far_piece(dz, r, dk):
    return (BLOCK[f"O{r}"], dz + 2 * dk)


def piece_id(piece):
    return piece[0] * CHUNKS + piece[1]


class Links:
    def __init__(self, store, send_sem, recv_sem, peers, depth):
        self.store, self.send_sem, self.recv_sem = store, send_sem, recv_sem
        self.peers, self.depth = peers, depth
        self.sends = {}

    def view(self, piece):
        return self.store.at[piece[0], pl.ds(piece[1] * self.depth, self.depth)]

    def send(self, source, piece, peer, key=None):
        copy = pltpu.make_async_remote_copy(
            src_ref=source,
            dst_ref=self.view(piece),
            send_sem=self.send_sem.at[self.sends.setdefault((piece, key or peer), len(self.sends))],
            recv_sem=self.recv_sem.at[piece_id(piece)],
            device_id=self.peers[peer],
            device_id_type=MESH,
        )
        copy.start()

    def forward(self, piece, target, peer, key=None):
        self.send(self.view(piece), target, peer, key)

    def any_copy(self, piece, send_sem, recv_sem):
        here = self.view(piece)
        return pltpu.make_async_remote_copy(
            src_ref=here,
            dst_ref=here,
            send_sem=send_sem,
            recv_sem=recv_sem,
            device_id=self.peers["core"],
            device_id_type=MESH,
        )

    def wait(self, piece):
        self.any_copy(piece, self.send_sem.at[0], self.recv_sem.at[piece_id(piece)]).wait_recv()

    def finish(self):
        for n in range(len(self.sends)):
            self.any_copy((0, 0), self.send_sem.at[n], self.recv_sem.at[0]).wait_send()


def half_step(store, turned, inter, total, t):
    electrons, basis = store.shape[2:]
    early, late = t < EARLY, t < 2 * EARLY
    g = jnp.where(late, jnp.where(early, 0, 1), lax.rem(t, 2))
    b = jnp.where(late, jnp.where(early, t, t - EARLY), t // 2)
    block = store.at[b]
    for n in range(turned.shape[2] // 256):
        for m in range(store.shape[1] // 4):
            vectors = block[4 * m : 4 * m + 4].reshape(4 * electrons, basis)
            made = jnp.dot(vectors, turned[g, :, n * 256 : (n + 1) * 256], preferred_element_type=jnp.float32)
            made = made.astype(jnp.bfloat16)
            for v in range(0, 4, 2):
                for s in range(0, 4, 2):
                    a = made[v * 64 : v * 64 + 64, s * 64 : s * 64 + 128]
                    c = made[v * 64 + 64 : v * 64 + 128, s * 64 : s * 64 + 128]
                    row, col = (4 * n + s) * 64, (4 * m + v) * 64
                    inter[row : row + 64, col : col + 128] = jnp.concatenate([a[:, :64], c[:, :64]], axis=1)
                    inter[row + 64 : row + 128, col : col + 128] = jnp.concatenate([a[:, 64:], c[:, 64:]], axis=1)
    for n in range(basis // 256):
        part = block[:, :, n * 256 : (n + 1) * 256].reshape(-1, 256)
        total[g, :, n * 256 : (n + 1) * 256] += jnp.dot(inter[...], part, preferred_element_type=jnp.float32)


def kernel(
    parents, counts, orbitals_hbm, cholesky_hbm, steps_hbm, energy_ref, grad_ref,
    store, orb, stp, out, slots, tag_out, tags, turned, total, inter, weights, e_out, e_in,
    load_sem, slot_send, slot_recv, tag_send, tag_recv, e_send, e_recv, piece_send, piece_recv,
):
    y, h, l, x, k = (lax.axis_index(name) for name in NAMES)
    per_device, electrons, basis = orb.shape
    depth = store.shape[1] // CHUNKS
    half = NY * CAP * electrons

    loads = [
        pltpu.make_async_copy(src, dst, load_sem.at[i])
        for i, (src, dst) in enumerate(((steps_hbm, stp), (cholesky_hbm, store.at[0]), (orbitals_hbm, orb)))
    ]
    for load in loads:
        load.start()

    up, down = {"x": lax.rem(x + 1, NX)}, {"x": lax.rem(x + NX - 1, NX)}
    peers = {
        "x+": up,
        "x-": down,
        "pair": {"l": 1 - l},
        "cross": {"h": 1 - h, "l": 1 - l},
        "core": {"k": 1 - k},
        "y+": {"y": lax.rem(y + 1, NY)},
        "y-": {"y": lax.rem(y + NY - 1, NY)},
    }
    walk_ids = range(1, len(REACH))
    walk_to = {n: {"y": lax.rem(y + REACH[n][1], NY), "h": lax.rem(h + REACH[n][0], NH)} for n in walk_ids}
    walk_from = {n: {"y": lax.rem(y + NY - REACH[n][1], NY), "h": lax.rem(h + REACH[n][0], NH)} for n in walk_ids}

    barrier = pltpu.get_barrier_semaphore()
    greeted = list(walk_to.values()) + [peers[p] for p in ("x+", "x-", "pair", "cross", "core")]
    for peer in greeted:
        pl.semaphore_signal(barrier, inc=1, device_id=peer, device_id_type=MESH)

    chol_walkers = 16 * per_device
    parent = [parents[0, j] for j in range(per_device)]
    owner = [p // chol_walkers for p in parent]
    keys = []
    for j in range(per_device):
        rank = sum([jnp.where(owner[i] == owner[j], 1, 0) for i in range(j)], jnp.int32(0))
        keys.append(owner[j] * CAP + rank)
    rows = lax.broadcasted_iota(jnp.int32, (per_device, 128), 0)
    loads[0].wait()
    walker_of, live_of = {}, {}
    for n, (dh, dy) in enumerate(REACH):
        device = lax.rem(y + dy, NY) * NH + lax.rem(h + dh, NH)
        for r in range(CAP):
            key = device * CAP + r
            index, mark, live = jnp.int32(0), jnp.int32(-1), jnp.int32(0)
            for j in range(per_device):
                hit = keys[j] == key
                alive = jnp.logical_and(hit, j < counts[0, 0])
                index = jnp.where(hit, j, index)
                mark = jnp.where(alive, parent[j] % per_device, mark)
                live = jnp.where(alive, 1, live)
            walker_of[n, r], live_of[n, r] = index, live
            tag = jnp.where(rows == mark, 1.0, 0.0).astype(jnp.float32)
            (out if n else slots)[n, r] = stp[index]
            (tag_out if n else tags)[n, r] = tag
    loads[1].wait()
    pl.semaphore_wait(barrier, len(greeted))

    def remote(source, target, send, recv, peer):
        return pltpu.make_async_remote_copy(
            src_ref=source, dst_ref=target, send_sem=send, recv_sem=recv, device_id=peer, device_id_type=MESH
        )

    tag_copies, slot_copies = {}, {}
    for n in walk_ids:
        tag_copies[n] = remote(tag_out.at[n], tags.at[n], tag_send.at[n], tag_recv.at[n], walk_to[n])
        slot_copies[n] = remote(out.at[n], slots.at[n], slot_send.at[n], slot_recv.at[n], walk_to[n])
        tag_copies[n].start()
        slot_copies[n].start()

    links = Links(store, piece_send, piece_recv, peers, depth)

    def own(i):
        return store.at[0, pl.ds(lax.rem(y + i, CHUNKS) * depth, depth)]

    for i in range(CHUNKS):
        links.send(own(i), (BLOCK["H1"], i), "core")
        links.send(own(i), x_piece(0, 0, i, 0), "x+")
        links.send(own(i), x_piece(0, 1, i, 0), "x-")
    links.send(own(1), pair_piece(1, 0), "pair")
    links.send(own(0), pair_piece(0, 0), "pair")
    links.send(own(2), pair_piece(2, 0), "cross")
    links.send(own(3), pair_piece(3, 0), "cross")

    def x_arrived(dz, i):
        for side in range(2):
            piece = x_piece(dz, side, i, 0)
            links.wait(piece)
            links.forward(piece, x_piece(dz, side, i, 1), "core")

    def first_x():
        x_arrived(0, 0)

        @pl.when(k == 0)
        def _():
            links.forward(x_piece(0, 0, 0, 0), far_piece(0, 0, 0), "x+", "x")

        @pl.when(k == 1)
        def _():
            links.forward(x_piece(0, 1, 0, 0), far_piece(0, 0, 0), "x-", "x")

        for side in range(2):
            links.forward(x_piece(0, side, 0, 0), x_piece(1, side, 0, 0), "cross")

    def pair_arrived(i):
        piece = pair_piece(i, 0)
        links.wait(piece)
        links.forward(piece, pair_piece(i, 1), "core")
        if i:
            links.forward(piece, x_piece(1, 0, i, 0), "x+")
            links.forward(piece, x_piece(1, 1, i, 0), "x-")

    def far_arrived(dz):
        piece = far_piece(dz, 0, 0)
        links.wait(piece)
        links.forward(piece, far_piece(dz, 0, 1), "core")
        links.forward(piece, far_piece(dz, 3, 0), "y+")
        links.forward(piece, far_piece(dz, 1, 0), "y-")
        if dz == 0:
            links.forward(piece, far_piece(1, 0, 0), "pair")

    def far_turned(dz):
        for r, onward in ((3, "y+"), (1, "y-")):
            piece = far_piece(dz, r, 0)
            links.wait(piece)
            links.forward(piece, far_piece(dz, r, 1), "core")
            if (dz == 0) == (r == 3):
                links.forward(piece, far_piece(dz, 2, 0), onward)

    def far_last(dz):
        piece = far_piece(dz, 2, 0)
        links.wait(piece)
        links.forward(piece, far_piece(dz, 2, 1), "core")

    events = [
        (1, first_x, ()),
        (3, x_arrived, (0, 1)),
        (4, x_arrived, (0, 2)),
        (6, pair_arrived, (1,)),
        (6, pair_arrived, (2,)),
        (7, x_arrived, (0, 3)),
        (10, pair_arrived, (0,)),
        (10, pair_arrived, (3,)),
        (11, far_arrived, (0,)),
        (14, x_arrived, (1, 1)),
        (16, far_arrived, (1,)),
        (17, far_turned, (0,)),
        (18, x_arrived, (1, 0)),
        (20, x_arrived, (1, 2)),
        (22, far_turned, (1,)),
        (24, x_arrived, (1, 3)),
        (25, far_last, (0,)),
        (28, far_last, (1,)),
    ]
    first_use = {}
    for place, name in enumerate(ORDER):
        first_use[name] = place if place < EARLY else 2 * place

    per_half = len(REACH) // 2

    def clones(g):
        for n in range(g * per_half, (g + 1) * per_half):
            if n:
                tag_copies[n].wait_recv()
                slot_copies[n].wait_recv()

        def one_slot(s, carry):
            n, r = g * per_half + s // CAP, s % CAP
            marks = [
                jnp.broadcast_to(tags[n, r, i : i + 1, :], (16, 128)).astype(jnp.bfloat16) for i in range(per_device)
            ]
            for top in range(0, electrons, 16):
                for left in range(0, basis, 128):
                    found = jnp.zeros((16, 128), jnp.bfloat16)
                    for i in range(per_device):
                        found += orb[i, top : top + 16, left : left + 128] * marks[i]
                    step = slots[n, r, top : top + 16, left : left + 128]
                    made = found.astype(jnp.float32) + step.astype(jnp.float32)
                    slots[n, r, top : top + 16, left : left + 128] = made.astype(jnp.bfloat16)
            return carry

        lax.fori_loop(0, per_half * CAP, one_slot, 0)
        turned[g] = slots[g * per_half : (g + 1) * per_half].reshape(half, basis).T

    loads[2].wait()
    clones(0)
    total[...] = jnp.zeros_like(total)

    at = {}
    for when, event, of in events:
        at.setdefault(when, []).append(functools.partial(event, *of))
    for name in ORDER[1:]:
        second = range(CHUNKS) if name == "H1" else (1, 3) if name[0] == "P" else (2, 3)
        for m in second:
            at.setdefault(first_use[name], []).append(functools.partial(links.wait, (BLOCK[name], m)))
    at.setdefault(EARLY, []).append(functools.partial(clones, 1))

    def dispatch(t, first, last):
        due = [when for when in at if first <= when < last]
        if not due:
            return
        if last - first == 1:
            for event in at[first]:
                event()
            return
        middle = (first + last) // 2
        if min(due) < middle:
            pl.when(t < middle)(lambda: dispatch(t, first, middle))
        if max(due) >= middle:
            pl.when(t >= middle)(lambda: dispatch(t, middle, last))

    def with_events(t, carry):
        dispatch(t, 0, 2 * len(ORDER))
        half_step(store, turned, inter, total, t)
        return carry

    lax.fori_loop(0, 2 * len(ORDER), with_events, jnp.int32(0))

    def energy_of(s, carry):
        n, r = s // CAP, s % CAP
        g = n // per_half
        base = pl.multiple_of(s % (per_half * CAP) * electrons, electrons)
        tile = jnp.zeros((8, 128), jnp.float32)
        for top in range(0, electrons, 16):
            for left in range(0, basis, 128):
                grad = total[g, pl.ds(base + top, 16), left : left + 128]
                made = slots[n, r, top : top + 16, left : left + 128].astype(jnp.float32) * grad
                tile += made[:8] + made[8:]
        e_out[n, r] = tile * -0.5
        return carry

    lax.fori_loop(0, len(REACH) * CAP, energy_of, 0)
    e_copies = {}
    for n in walk_ids:
        e_copies[n] = remote(e_out.at[n], e_in.at[n], e_send.at[n], e_recv.at[n], walk_from[n])
        e_copies[n].start()

    for n in range(len(REACH)):
        for r in range(CAP):
            for i in range(per_device):
                weights[n * CAP + r, i] = jnp.broadcast_to(-tags[n, r, i : i + 1, :], (8, 128))

    def gather(t, carry):
        top = pl.multiple_of(t // 8 * 8, 8)
        left = pl.multiple_of(t % 8 * 128, 128)
        sums = [jnp.zeros((8, 128), jnp.float32) for _ in range(per_device)]
        for s in range(len(REACH) * CAP):
            g, first = s // (per_half * CAP), s % (per_half * CAP) * electrons
            grad = total[g, pl.ds(first + top, 8), pl.ds(left, 128)]
            for i in range(per_device):
                sums[i] += weights[s, i] * grad
        for i in range(per_device):
            grad_ref[i, pl.ds(top, 8), pl.ds(left, 128)] = sums[i]
        return carry

    lax.fori_loop(0, electrons * basis // 1024, gather, 0)

    for n in walk_ids:
        e_copies[n].wait()
    for j in range(per_device):
        tile = jnp.zeros((8, 128), jnp.float32)
        for n in range(len(REACH)):
            for r in range(CAP):
                used = jnp.logical_and(walker_of[n, r] == j, live_of[n, r] == 1)
                tile += jnp.where(used, 1.0, 0.0).astype(jnp.float32) * (e_in if n else e_out)[n, r]
        energy_ref[j] = tile

    for n in walk_ids:
        tag_copies[n].wait_send()
        slot_copies[n].wait_send()
    links.finish()


def body(orbitals, cholesky, parents, counts, steps):
    per_device, electrons, basis = orbitals.shape
    vectors = cholesky.shape[0]
    half = NY * CAP * electrons
    reach = len(REACH)
    f32, bf16 = jnp.float32, jnp.bfloat16
    dma = pltpu.SemaphoreType.DMA
    energy, grad = pl.pallas_call(
        kernel,
        out_shape=(
            jax.ShapeDtypeStruct((per_device, 8, 128), f32),
            jax.ShapeDtypeStruct((per_device, electrons, basis), f32),
        ),
        in_specs=[pl.BlockSpec(memory_space=pltpu.SMEM)] * 2 + [pl.BlockSpec(memory_space=pl.ANY)] * 3,
        out_specs=(pl.BlockSpec(memory_space=pltpu.VMEM), pl.BlockSpec(memory_space=pltpu.VMEM)),
        scratch_shapes=[
            pltpu.VMEM((len(ORDER), vectors, electrons, basis), bf16),
            pltpu.VMEM((per_device, electrons, basis), bf16),
            pltpu.VMEM((per_device, electrons, basis), bf16),
            pltpu.VMEM((reach, CAP, electrons, basis), bf16),
            pltpu.VMEM((reach, CAP, electrons, basis), bf16),
            pltpu.VMEM((reach, CAP, per_device, 128), f32),
            pltpu.VMEM((reach, CAP, per_device, 128), f32),
            pltpu.VMEM((2, basis, half), bf16),
            pltpu.VMEM((2, half, basis), f32),
            pltpu.VMEM((half, vectors * electrons), bf16),
            pltpu.VMEM((reach * CAP, per_device, 8, 128), f32),
            pltpu.VMEM((reach, CAP, 8, 128), f32),
            pltpu.VMEM((reach, CAP, 8, 128), f32),
            dma((3,)),
            *[dma((reach,))] * 6,
            dma((64,)),
            dma((len(ORDER) * CHUNKS,)),
        ],
        compiler_params=pltpu.CompilerParams(
            collective_id=0, has_side_effects=True, vmem_limit_bytes=60 * 2**20
        ),
        name="exchange",
    )(parents.reshape(1, -1), counts, orbitals, cholesky, steps)
    return jnp.sum(energy, axis=(1, 2)), grad


def solution(mesh):
    torus = Mesh(mesh.devices.reshape(NY, NH, 2, NX, 2), NAMES)
    return jax.shard_map(
        body,
        mesh=torus,
        in_specs=(
            P(NAMES, None, None),
            P(("l", "x", "k"), None, None),
            P(NAMES),
            P(("y", "h"), ("l", "x", "k")),
            P(NAMES, None, None),
        ),
        out_specs=(P(NAMES), P(NAMES, None, None)),
        check_vma=False,
    )
```

```python
import functools

import jax
import jax.numpy as jnp
from jax import lax
from jax.experimental import pallas as pl
from jax.experimental.pallas import tpu as pltpu
from jax.sharding import Mesh
from jax.sharding import PartitionSpec as P

NAMES = ("y", "h", "l", "x", "k")
MESH = pl.DeviceIdType.MESH
CAP = 2
NY, NH, NX = 4, 2, 4
CHUNKS = 4
EARLY = 4

REACH = ((0, 0), (0, 1), (0, 3), (1, 0), (0, 2), (1, 1), (1, 3), (1, 2))

ORDER = ("H0", "H1", "X00", "X01", "X02", "X03", "P1", "P0", "X11", "O0", "X10", "X12", "O1", "X13", "O3", "O2")
BLOCK = {name: i for i, name in enumerate(ORDER)}


def pair_piece(i, dk):
    return (BLOCK[f"P{i // 2}"], (i % 2) * 2 + dk)


def x_piece(dz, side, i, dk):
    return (BLOCK[f"X{dz}{i}"], side + 2 * dk)


def far_piece(dz, r, dk):
    return (BLOCK[f"O{r}"], dz + 2 * dk)


def piece_id(piece):
    return piece[0] * CHUNKS + piece[1]


class Links:
    def __init__(self, store, send_sem, recv_sem, peers, depth):
        self.store, self.send_sem, self.recv_sem = store, send_sem, recv_sem
        self.peers, self.depth = peers, depth
        self.sends = {}

    def view(self, piece):
        return self.store.at[piece[0], pl.ds(piece[1] * self.depth, self.depth)]

    def send(self, source, piece, peer, key=None):
        copy = pltpu.make_async_remote_copy(
            src_ref=source,
            dst_ref=self.view(piece),
            send_sem=self.send_sem.at[self.sends.setdefault((piece, key or peer), len(self.sends))],
            recv_sem=self.recv_sem.at[piece_id(piece)],
            device_id=self.peers[peer],
            device_id_type=MESH,
        )
        copy.start()

    def forward(self, piece, target, peer, key=None):
        self.send(self.view(piece), target, peer, key)

    def any_copy(self, piece, send_sem, recv_sem):
        here = self.view(piece)
        return pltpu.make_async_remote_copy(
            src_ref=here,
            dst_ref=here,
            send_sem=send_sem,
            recv_sem=recv_sem,
            device_id=self.peers["core"],
            device_id_type=MESH,
        )

    def wait(self, piece):
        self.any_copy(piece, self.send_sem.at[0], self.recv_sem.at[piece_id(piece)]).wait_recv()

    def finish(self):
        for n in range(len(self.sends)):
            self.any_copy((0, 0), self.send_sem.at[n], self.recv_sem.at[0]).wait_send()


def meet(block, turned, inter, g):
    electrons = block.shape[1]
    for n in range(turned.shape[2] // 256):
        for m in range(block.shape[0] // 4):
            vectors = block[4 * m : 4 * m + 4].reshape(4 * electrons, -1)
            made = jnp.dot(vectors, turned[g, :, n * 256 : (n + 1) * 256], preferred_element_type=jnp.float32)
            made = made.astype(jnp.bfloat16)
            for v in range(0, 4, 2):
                for s in range(0, 4, 2):
                    a = made[v * 64 : v * 64 + 64, s * 64 : s * 64 + 128]
                    c = made[v * 64 + 64 : v * 64 + 128, s * 64 : s * 64 + 128]
                    row, col = (4 * n + s) * 64, (4 * m + v) * 64
                    inter[g, row : row + 64, col : col + 128] = jnp.concatenate([a[:, :64], c[:, :64]], axis=1)
                    inter[g, row + 64 : row + 128, col : col + 128] = jnp.concatenate([a[:, 64:], c[:, 64:]], axis=1)


def spread(block, inter, total, g):
    for n in range(block.shape[2] // 256):
        part = block[:, :, n * 256 : (n + 1) * 256].reshape(-1, 256)
        total[g, :, n * 256 : (n + 1) * 256] += jnp.dot(inter[g], part, preferred_element_type=jnp.float32)


def kernel(
    parents, counts, orbitals_hbm, cholesky_hbm, steps_hbm, energy_ref, grad_ref,
    store, orb, stp, out, slots, tag_out, tags, turned, total, inter, weights, made_grad, e_out, e_in,
    load_sem, slot_send, slot_recv, tag_send, tag_recv, e_send, e_recv, piece_send, piece_recv,
):
    y, h, l, x, k = (lax.axis_index(name) for name in NAMES)
    per_device, electrons, basis = orb.shape
    depth = store.shape[1] // CHUNKS
    half = NY * CAP * electrons

    loads = [
        pltpu.make_async_copy(src, dst, load_sem.at[i])
        for i, (src, dst) in enumerate(((steps_hbm, stp), (cholesky_hbm, store.at[0]), (orbitals_hbm, orb)))
    ]
    for load in loads:
        load.start()

    up, down = {"x": lax.rem(x + 1, NX)}, {"x": lax.rem(x + NX - 1, NX)}
    peers = {
        "x+": up,
        "x-": down,
        "pair": {"l": 1 - l},
        "cross": {"h": 1 - h, "l": 1 - l},
        "core": {"k": 1 - k},
        "y+": {"y": lax.rem(y + 1, NY)},
        "y-": {"y": lax.rem(y + NY - 1, NY)},
    }
    walk_ids = range(1, len(REACH))
    walk_to = {n: {"y": lax.rem(y + REACH[n][1], NY), "h": lax.rem(h + REACH[n][0], NH)} for n in walk_ids}
    walk_from = {n: {"y": lax.rem(y + NY - REACH[n][1], NY), "h": lax.rem(h + REACH[n][0], NH)} for n in walk_ids}

    barrier = pltpu.get_barrier_semaphore()
    greeted = list(walk_to.values()) + [peers[p] for p in ("x+", "x-", "pair", "cross", "core")]
    for peer in greeted:
        pl.semaphore_signal(barrier, inc=1, device_id=peer, device_id_type=MESH)

    chol_walkers = 16 * per_device
    parent = [parents[0, j] for j in range(per_device)]
    owner = [p // chol_walkers for p in parent]
    keys = []
    for j in range(per_device):
        rank = sum([jnp.where(owner[i] == owner[j], 1, 0) for i in range(j)], jnp.int32(0))
        keys.append(owner[j] * CAP + rank)
    rows = lax.broadcasted_iota(jnp.int32, (per_device, 128), 0)
    loads[0].wait()
    walker_of, live_of = {}, {}
    for n, (dh, dy) in enumerate(REACH):
        device = lax.rem(y + dy, NY) * NH + lax.rem(h + dh, NH)
        for r in range(CAP):
            key = device * CAP + r
            index, mark, live = jnp.int32(0), jnp.int32(-1), jnp.int32(0)
            for j in range(per_device):
                hit = keys[j] == key
                alive = jnp.logical_and(hit, j < counts[0, 0])
                index = jnp.where(hit, j, index)
                mark = jnp.where(alive, parent[j] % per_device, mark)
                live = jnp.where(alive, 1, live)
            walker_of[n, r], live_of[n, r] = index, live
            tag = jnp.where(rows == mark, 1.0, 0.0).astype(jnp.float32)
            (out if n else slots)[n, r] = stp[index]
            (tag_out if n else tags)[n, r] = tag
    loads[1].wait()
    pl.semaphore_wait(barrier, len(greeted))

    def remote(source, target, send, recv, peer):
        return pltpu.make_async_remote_copy(
            src_ref=source, dst_ref=target, send_sem=send, recv_sem=recv, device_id=peer, device_id_type=MESH
        )

    tag_copies, slot_copies = {}, {}
    for n in walk_ids:
        tag_copies[n] = remote(tag_out.at[n], tags.at[n], tag_send.at[n], tag_recv.at[n], walk_to[n])
        slot_copies[n] = remote(out.at[n], slots.at[n], slot_send.at[n], slot_recv.at[n], walk_to[n])
        tag_copies[n].start()
        slot_copies[n].start()

    links = Links(store, piece_send, piece_recv, peers, depth)

    def own(i):
        return store.at[0, pl.ds(lax.rem(y + i, CHUNKS) * depth, depth)]

    for i in range(CHUNKS):
        links.send(own(i), (BLOCK["H1"], i), "core")
        links.send(own(i), x_piece(0, 0, i, 0), "x+")
        links.send(own(i), x_piece(0, 1, i, 0), "x-")
    links.send(own(1), pair_piece(1, 0), "pair")
    links.send(own(0), pair_piece(0, 0), "pair")
    links.send(own(2), pair_piece(2, 0), "cross")
    links.send(own(3), pair_piece(3, 0), "cross")

    def x_arrived(dz, i):
        for side in range(2):
            piece = x_piece(dz, side, i, 0)
            links.wait(piece)
            links.forward(piece, x_piece(dz, side, i, 1), "core")

    def first_x():
        x_arrived(0, 0)

        @pl.when(k == 0)
        def _():
            links.forward(x_piece(0, 0, 0, 0), far_piece(0, 0, 0), "x+", "x")

        @pl.when(k == 1)
        def _():
            links.forward(x_piece(0, 1, 0, 0), far_piece(0, 0, 0), "x-", "x")

        for side in range(2):
            links.forward(x_piece(0, side, 0, 0), x_piece(1, side, 0, 0), "cross")

    def pair_arrived(i):
        piece = pair_piece(i, 0)
        links.wait(piece)
        links.forward(piece, pair_piece(i, 1), "core")
        if i:
            links.forward(piece, x_piece(1, 0, i, 0), "x+")
            links.forward(piece, x_piece(1, 1, i, 0), "x-")

    def far_arrived(dz):
        piece = far_piece(dz, 0, 0)
        links.wait(piece)
        links.forward(piece, far_piece(dz, 0, 1), "core")
        links.forward(piece, far_piece(dz, 3, 0), "y+")
        links.forward(piece, far_piece(dz, 1, 0), "y-")
        if dz == 0:
            links.forward(piece, far_piece(1, 0, 0), "pair")

    def far_turned(dz):
        for r, onward in ((3, "y+"), (1, "y-")):
            piece = far_piece(dz, r, 0)
            links.wait(piece)
            links.forward(piece, far_piece(dz, r, 1), "core")
            if (dz == 0) == (r == 3):
                links.forward(piece, far_piece(dz, 2, 0), onward)

    def far_last(dz):
        piece = far_piece(dz, 2, 0)
        links.wait(piece)
        links.forward(piece, far_piece(dz, 2, 1), "core")

    events = [
        (1, first_x, ()),
        (3, x_arrived, (0, 1)),
        (4, x_arrived, (0, 2)),
        (6, pair_arrived, (1,)),
        (6, pair_arrived, (2,)),
        (8, x_arrived, (0, 3)),
        (11, pair_arrived, (0,)),
        (11, pair_arrived, (3,)),
        (12, far_arrived, (0,)),
        (15, x_arrived, (1, 1)),
        (16, far_arrived, (1,)),
        (17, far_turned, (0,)),
        (19, x_arrived, (1, 0)),
        (20, x_arrived, (1, 2)),
        (22, far_turned, (1,)),
        (23, x_arrived, (1, 3)),
        (26, far_last, (0,)),
        (28, far_last, (1,)),
    ]
    first_use = {}
    for place, name in enumerate(ORDER):
        first_use[name] = place if place < EARLY else 2 * place

    per_half = len(REACH) // 2

    def clones(g):
        for place in range(per_half):
            n = g * per_half + place
            if n:
                tag_copies[n].wait_recv()
                slot_copies[n].wait_recv()

            def one_slot(r, carry, n=n):
                marks = [
                    jnp.broadcast_to(tags[n, r, i : i + 1, :], (16, 128)).astype(jnp.bfloat16)
                    for i in range(per_device)
                ]
                for top in range(0, electrons, 16):
                    for left in range(0, basis, 128):
                        found = jnp.zeros((16, 128), jnp.bfloat16)
                        for i in range(per_device):
                            found += orb[i, top : top + 16, left : left + 128] * marks[i]
                        step = slots[n, r, top : top + 16, left : left + 128]
                        made = found.astype(jnp.float32) + step.astype(jnp.float32)
                        slots[n, r, top : top + 16, left : left + 128] = made.astype(jnp.bfloat16)
                return carry

            lax.fori_loop(0, CAP, one_slot, 0)
            wide = CAP * electrons
            turned[g, :, place * wide : (place + 1) * wide] = slots[n].reshape(wide, basis).T

    loads[2].wait()
    clones(0)
    total[...] = jnp.zeros_like(total)

    at = {}
    for when, event, of in events:
        at.setdefault(when, []).append(functools.partial(event, *of))
    for name in ORDER[1:]:
        second = range(CHUNKS) if name == "H1" else (1, 3) if name[0] == "P" else (2, 3)
        for m in second:
            at.setdefault(first_use[name], []).append(functools.partial(links.wait, (BLOCK[name], m)))
    at.setdefault(EARLY, []).append(functools.partial(clones, 1))

    e_copies = {
        n: remote(e_out.at[n], e_in.at[n], e_send.at[n], e_recv.at[n], walk_from[n]) for n in walk_ids
    }

    def energies(g):
        def energy_of(s, carry):
            n, r = s // CAP, s % CAP
            base = pl.multiple_of(s % (per_half * CAP) * electrons, electrons)
            tile = jnp.zeros((8, 128), jnp.float32)
            for top in range(0, electrons, 16):
                for left in range(0, basis, 128):
                    grad = total[g, pl.ds(base + top, 16), left : left + 128]
                    made = slots[n, r, top : top + 16, left : left + 128].astype(jnp.float32) * grad
                    tile += made[:8] + made[8:]
            e_out[n, r] = tile * -0.5
            return carry

        lax.fori_loop(g * per_half * CAP, (g + 1) * per_half * CAP, energy_of, 0)
        for n in range(g * per_half, (g + 1) * per_half):
            if n:
                e_copies[n].start()

    at.setdefault(2 * len(ORDER) - 1, []).append(functools.partial(energies, 1))

    def dispatch(t, at, first, last):
        due = [when for when in at if first <= when < last]
        if not due:
            return
        if last - first == 1:
            for event in at[first]:
                event()
            return
        middle = (first + last) // 2
        if min(due) < middle:
            pl.when(t < middle)(lambda: dispatch(t, at, first, middle))
        if max(due) >= middle:
            pl.when(t >= middle)(lambda: dispatch(t, at, middle, last))

    def half_step(t, carry):
        dispatch(t, at, 0, 2 * EARLY)
        g = jnp.where(t < EARLY, 0, 1)
        block = store.at[jnp.where(t < EARLY, t, t - EARLY)]
        meet(block, turned, inter, g)
        spread(block, inter, total, g)
        return carry

    opening = {when // 2: at[when] for when in at if when >= 2 * EARLY and when % 2 == 0}
    middle = {when // 2: at[when] for when in at if when >= 2 * EARLY and when % 2 == 1}

    def full_step(b, carry):
        dispatch(b, opening, EARLY, len(ORDER))
        block = store.at[b]
        meet(block, turned, inter, 1)
        meet(block, turned, inter, 0)
        spread(block, inter, total, 1)
        dispatch(b, middle, EARLY, len(ORDER))
        spread(block, inter, total, 0)
        return carry

    lax.fori_loop(0, 2 * EARLY, half_step, jnp.int32(0))
    lax.fori_loop(EARLY, len(ORDER), full_step, jnp.int32(0))

    energies(0)
    for n in range(len(REACH)):
        for r in range(CAP):
            for i in range(per_device):
                weights[n * CAP + r, i] = jnp.broadcast_to(-tags[n, r, i : i + 1, :], (8, 128))

    def gather(t, carry):
        top = pl.multiple_of(t // 8 * 8, 8)
        left = pl.multiple_of(t % 8 * 128, 128)
        sums = [jnp.zeros((8, 128), jnp.float32) for _ in range(per_device)]
        for s in range(len(REACH) * CAP):
            g, first = s // (per_half * CAP), s % (per_half * CAP) * electrons
            grad = total[g, pl.ds(first + top, 8), pl.ds(left, 128)]
            for i in range(per_device):
                sums[i] += weights[s, i] * grad
        for i in range(per_device):
            made_grad[i, pl.ds(top, 8), pl.ds(left, 128)] = sums[i]
        return carry

    lax.fori_loop(0, electrons * basis // 1024, gather, 0)

    store_grad = pltpu.make_async_copy(made_grad, grad_ref, load_sem.at[0])
    store_grad.start()
    for n in walk_ids:
        tag_copies[n].wait_send()
        slot_copies[n].wait_send()
    links.finish()
    for n in walk_ids:
        e_copies[n].wait()
    for j in range(per_device):
        tile = jnp.zeros((8, 128), jnp.float32)
        for n in range(len(REACH)):
            for r in range(CAP):
                used = jnp.logical_and(walker_of[n, r] == j, live_of[n, r] == 1)
                tile += jnp.where(used, 1.0, 0.0).astype(jnp.float32) * (e_in if n else e_out)[n, r]
        energy_ref[j] = tile

    store_grad.wait()


def finish(parts_ref, grad_ref, energy_ref, out_ref):
    out_ref[...] = grad_ref[...]

    @pl.when(pl.program_id(0) == 0)
    def _():
        lanes = lax.broadcasted_iota(jnp.int32, energy_ref.shape, 1)
        row = jnp.zeros(energy_ref.shape, jnp.float32)
        for j in range(parts_ref.shape[0]):
            row = jnp.where(lanes == j, jnp.sum(parts_ref[j]), row)
        energy_ref[...] = row


def body(orbitals, cholesky, parents, counts, steps):
    per_device, electrons, basis = orbitals.shape
    vectors = cholesky.shape[0]
    half = NY * CAP * electrons
    reach = len(REACH)
    f32, bf16 = jnp.float32, jnp.bfloat16
    dma = pltpu.SemaphoreType.DMA
    energy, grad = pl.pallas_call(
        kernel,
        out_shape=(
            jax.ShapeDtypeStruct((per_device, 8, 128), f32),
            jax.ShapeDtypeStruct((per_device, electrons, basis), f32),
        ),
        in_specs=[pl.BlockSpec(memory_space=pltpu.SMEM)] * 2 + [pl.BlockSpec(memory_space=pl.ANY)] * 3,
        out_specs=(pl.BlockSpec(memory_space=pltpu.VMEM), pl.BlockSpec(memory_space=pl.ANY)),
        scratch_shapes=[
            pltpu.VMEM((len(ORDER), vectors, electrons, basis), bf16),
            pltpu.VMEM((per_device, electrons, basis), bf16),
            pltpu.VMEM((per_device, electrons, basis), bf16),
            pltpu.VMEM((reach, CAP, electrons, basis), bf16),
            pltpu.VMEM((reach, CAP, electrons, basis), bf16),
            pltpu.VMEM((reach, CAP, per_device, 128), f32),
            pltpu.VMEM((reach, CAP, per_device, 128), f32),
            pltpu.VMEM((2, basis, half), bf16),
            pltpu.VMEM((2, half, basis), f32),
            pltpu.VMEM((2, half, vectors * electrons), bf16),
            pltpu.VMEM((reach * CAP, per_device, 8, 128), f32),
            pltpu.VMEM((per_device, electrons, basis), f32),
            pltpu.VMEM((reach, CAP, 8, 128), f32),
            pltpu.VMEM((reach, CAP, 8, 128), f32),
            dma((3,)),
            *[dma((reach,))] * 6,
            dma((64,)),
            dma((len(ORDER) * CHUNKS,)),
        ],
        compiler_params=pltpu.CompilerParams(
            collective_id=0, has_side_effects=True, vmem_limit_bytes=60 * 2**20
        ),
        name="exchange",
    )(parents.reshape(1, -1), counts, orbitals, cholesky, steps)
    part = per_device // 4
    grad_spec = pl.BlockSpec((part, electrons, basis), lambda i: (i, 0, 0))
    energy, grad = pl.pallas_call(
        finish,
        grid=(4,),
        out_shape=(jax.ShapeDtypeStruct((1, per_device), f32), jax.ShapeDtypeStruct(grad.shape, f32)),
        in_specs=[pl.BlockSpec((per_device, 8, 128), lambda i: (0, 0, 0)), grad_spec],
        out_specs=(pl.BlockSpec((1, per_device), lambda i: (0, 0)), grad_spec),
        name="finish",
    )(energy, grad)
    return energy.reshape(per_device), grad


def solution(mesh):
    torus = Mesh(mesh.devices.reshape(NY, NH, 2, NX, 2), NAMES)
    return jax.shard_map(
        body,
        mesh=torus,
        in_specs=(
            P(NAMES, None, None),
            P(("l", "x", "k"), None, None),
            P(NAMES),
            P(("y", "h"), ("l", "x", "k")),
            P(NAMES, None, None),
        ),
        out_specs=(P(NAMES), P(NAMES, None, None)),
        check_vma=False,
    )
```

```python
import functools

import jax
import jax.numpy as jnp
from jax import lax
from jax.experimental import pallas as pl
from jax.experimental.pallas import tpu as pltpu
from jax.sharding import Mesh
from jax.sharding import PartitionSpec as P

NAMES = ("y", "h", "l", "x", "k")
MESH = pl.DeviceIdType.MESH
CAP = 2
NY, NH, NX = 4, 2, 4
CHUNKS = 4
EARLY = 4

REACH = ((0, 0), (0, 1), (0, 3), (1, 0), (0, 2), (1, 1), (1, 3), (1, 2))

ORDER = ("H0", "H1", "X00", "X01", "X02", "X03", "P1", "P0", "X11", "O0", "X10", "X12", "O1", "X13", "O3", "O2")
BLOCK = {name: i for i, name in enumerate(ORDER)}


def pair_piece(i, dk):
    return (BLOCK[f"P{i // 2}"], (i % 2) * 2 + dk)


def x_piece(dz, side, i, dk):
    return (BLOCK[f"X{dz}{i}"], side + 2 * dk)


def far_piece(dz, r, dk):
    return (BLOCK[f"O{r}"], dz + 2 * dk)


def piece_id(piece):
    return piece[0] * CHUNKS + piece[1]


class Links:
    def __init__(self, store, send_sem, recv_sem, peers, depth):
        self.store, self.send_sem, self.recv_sem = store, send_sem, recv_sem
        self.peers, self.depth = peers, depth
        self.sends = {}

    def view(self, piece):
        return self.store.at[piece[0], pl.ds(piece[1] * self.depth, self.depth)]

    def send(self, source, piece, peer, key=None):
        copy = pltpu.make_async_remote_copy(
            src_ref=source,
            dst_ref=self.view(piece),
            send_sem=self.send_sem.at[self.sends.setdefault((piece, key or peer), len(self.sends))],
            recv_sem=self.recv_sem.at[piece_id(piece)],
            device_id=self.peers[peer],
            device_id_type=MESH,
        )
        copy.start()

    def forward(self, piece, target, peer, key=None):
        self.send(self.view(piece), target, peer, key)

    def any_copy(self, piece, send_sem, recv_sem):
        here = self.view(piece)
        return pltpu.make_async_remote_copy(
            src_ref=here,
            dst_ref=here,
            send_sem=send_sem,
            recv_sem=recv_sem,
            device_id=self.peers["core"],
            device_id_type=MESH,
        )

    def wait(self, piece):
        self.any_copy(piece, self.send_sem.at[0], self.recv_sem.at[piece_id(piece)]).wait_recv()

    def finish(self):
        for n in range(len(self.sends)):
            self.any_copy((0, 0), self.send_sem.at[n], self.recv_sem.at[0]).wait_send()


def meet(block, turned, inter, g):
    electrons = block.shape[1]
    for n in range(turned.shape[2] // 256):
        for m in range(block.shape[0] // 4):
            vectors = block[4 * m : 4 * m + 4].reshape(4 * electrons, -1)
            made = jnp.dot(vectors, turned[g, :, n * 256 : (n + 1) * 256], preferred_element_type=jnp.float32)
            made = made.astype(jnp.bfloat16)
            for v in range(0, 4, 2):
                for s in range(0, 4, 2):
                    a = made[v * 64 : v * 64 + 64, s * 64 : s * 64 + 128]
                    c = made[v * 64 + 64 : v * 64 + 128, s * 64 : s * 64 + 128]
                    row, col = (4 * n + s) * 64, (4 * m + v) * 64
                    inter[g, row : row + 64, col : col + 128] = jnp.concatenate([a[:, :64], c[:, :64]], axis=1)
                    inter[g, row + 64 : row + 128, col : col + 128] = jnp.concatenate([a[:, 64:], c[:, 64:]], axis=1)


def spread(block, inter, total, g):
    for n in range(block.shape[2] // 256):
        part = block[:, :, n * 256 : (n + 1) * 256].reshape(-1, 256)
        total[g, :, n * 256 : (n + 1) * 256] += jnp.dot(inter[g], part, preferred_element_type=jnp.float32)


def kernel(
    parents, counts, orbitals_hbm, cholesky_hbm, steps_hbm, energy_ref, grad_ref,
    store, orb, stp, out, slots, tag_out, tags, turned, total, inter, weights, made_grad, e_out, e_in,
    load_sem, slot_send, slot_recv, tag_send, tag_recv, e_send, e_recv, piece_send, piece_recv,
):
    y, h, l, x, k = (lax.axis_index(name) for name in NAMES)
    per_device, electrons, basis = orb.shape
    depth = store.shape[1] // CHUNKS
    half = NY * CAP * electrons

    loads = [
        pltpu.make_async_copy(src, dst, load_sem.at[i])
        for i, (src, dst) in enumerate(((steps_hbm, stp), (cholesky_hbm, store.at[0]), (orbitals_hbm, orb)))
    ]
    for load in loads:
        load.start()

    up, down = {"x": lax.rem(x + 1, NX)}, {"x": lax.rem(x + NX - 1, NX)}
    peers = {
        "x+": up,
        "x-": down,
        "pair": {"l": 1 - l},
        "cross": {"h": 1 - h, "l": 1 - l},
        "core": {"k": 1 - k},
        "y+": {"y": lax.rem(y + 1, NY)},
        "y-": {"y": lax.rem(y + NY - 1, NY)},
    }
    walk_ids = range(1, len(REACH))
    walk_to = {n: {"y": lax.rem(y + REACH[n][1], NY), "h": lax.rem(h + REACH[n][0], NH)} for n in walk_ids}
    walk_from = {n: {"y": lax.rem(y + NY - REACH[n][1], NY), "h": lax.rem(h + REACH[n][0], NH)} for n in walk_ids}

    barrier = pltpu.get_barrier_semaphore()
    greeted = list(walk_to.values()) + [peers[p] for p in ("x+", "x-", "pair", "cross", "core")]
    for peer in greeted:
        pl.semaphore_signal(barrier, inc=1, device_id=peer, device_id_type=MESH)

    chol_walkers = 16 * per_device
    parent = [parents[0, j] for j in range(per_device)]
    owner = [p // chol_walkers for p in parent]
    keys = []
    for j in range(per_device):
        rank = sum([jnp.where(owner[i] == owner[j], 1, 0) for i in range(j)], jnp.int32(0))
        keys.append(owner[j] * CAP + rank)
    rows = lax.broadcasted_iota(jnp.int32, (per_device, 128), 0)
    loads[0].wait()
    walker_of, live_of = {}, {}
    for n, (dh, dy) in enumerate(REACH):
        device = lax.rem(y + dy, NY) * NH + lax.rem(h + dh, NH)
        for r in range(CAP):
            key = device * CAP + r
            index, mark, live = jnp.int32(0), jnp.int32(-1), jnp.int32(0)
            for j in range(per_device):
                hit = keys[j] == key
                alive = jnp.logical_and(hit, j < counts[0, 0])
                index = jnp.where(hit, j, index)
                mark = jnp.where(alive, parent[j] % per_device, mark)
                live = jnp.where(alive, 1, live)
            walker_of[n, r], live_of[n, r] = index, live
            tag = jnp.where(rows == mark, 1.0, 0.0).astype(jnp.float32)
            (out if n else slots)[n, r] = stp[index]
            (tag_out if n else tags)[n, r] = tag
    loads[1].wait()
    pl.semaphore_wait(barrier, len(greeted))

    def remote(source, target, send, recv, peer):
        return pltpu.make_async_remote_copy(
            src_ref=source, dst_ref=target, send_sem=send, recv_sem=recv, device_id=peer, device_id_type=MESH
        )

    tag_copies, slot_copies = {}, {}
    for n in walk_ids:
        tag_copies[n] = remote(tag_out.at[n], tags.at[n], tag_send.at[n], tag_recv.at[n], walk_to[n])
        slot_copies[n] = remote(out.at[n], slots.at[n], slot_send.at[n], slot_recv.at[n], walk_to[n])
        tag_copies[n].start()
        slot_copies[n].start()

    links = Links(store, piece_send, piece_recv, peers, depth)

    def own(i):
        return store.at[0, pl.ds(lax.rem(y + i, CHUNKS) * depth, depth)]

    for i in range(CHUNKS):
        links.send(own(i), (BLOCK["H1"], i), "core")
        links.send(own(i), x_piece(0, 0, i, 0), "x+")
        links.send(own(i), x_piece(0, 1, i, 0), "x-")
    links.send(own(1), pair_piece(1, 0), "pair")
    links.send(own(0), pair_piece(0, 0), "pair")
    links.send(own(2), pair_piece(2, 0), "cross")
    links.send(own(3), pair_piece(3, 0), "cross")

    def x_arrived(dz, i):
        for side in range(2):
            piece = x_piece(dz, side, i, 0)
            links.wait(piece)
            links.forward(piece, x_piece(dz, side, i, 1), "core")

    def first_x():
        x_arrived(0, 0)

        @pl.when(k == 0)
        def _():
            links.forward(x_piece(0, 0, 0, 0), far_piece(0, 0, 0), "x+", "x")

        @pl.when(k == 1)
        def _():
            links.forward(x_piece(0, 1, 0, 0), far_piece(0, 0, 0), "x-", "x")

        for side in range(2):
            links.forward(x_piece(0, side, 0, 0), x_piece(1, side, 0, 0), "cross")

    def pair_arrived(i):
        piece = pair_piece(i, 0)
        links.wait(piece)
        links.forward(piece, pair_piece(i, 1), "core")
        if i:
            links.forward(piece, x_piece(1, 0, i, 0), "x+")
            links.forward(piece, x_piece(1, 1, i, 0), "x-")

    def far_arrived(dz):
        piece = far_piece(dz, 0, 0)
        links.wait(piece)
        links.forward(piece, far_piece(dz, 0, 1), "core")
        links.forward(piece, far_piece(dz, 3, 0), "y+")
        links.forward(piece, far_piece(dz, 1, 0), "y-")
        if dz == 0:
            links.forward(piece, far_piece(1, 0, 0), "pair")

    def far_turned(dz):
        for r, onward in ((3, "y+"), (1, "y-")):
            piece = far_piece(dz, r, 0)
            links.wait(piece)
            links.forward(piece, far_piece(dz, r, 1), "core")
            if (dz == 0) == (r == 3):
                links.forward(piece, far_piece(dz, 2, 0), onward)

    def far_last(dz):
        piece = far_piece(dz, 2, 0)
        links.wait(piece)
        links.forward(piece, far_piece(dz, 2, 1), "core")

    events = [
        (1, first_x, ()),
        (3, x_arrived, (0, 1)),
        (4, x_arrived, (0, 2)),
        (6, pair_arrived, (1,)),
        (6, pair_arrived, (2,)),
        (8, x_arrived, (0, 3)),
        (11, pair_arrived, (0,)),
        (11, pair_arrived, (3,)),
        (12, far_arrived, (0,)),
        (15, x_arrived, (1, 1)),
        (16, far_arrived, (1,)),
        (17, far_turned, (0,)),
        (18, x_arrived, (1, 0)),
        (20, x_arrived, (1, 2)),
        (22, far_turned, (1,)),
        (23, x_arrived, (1, 3)),
        (26, far_last, (0,)),
        (28, far_last, (1,)),
    ]
    first_use = {}
    for place, name in enumerate(ORDER):
        first_use[name] = place if place < EARLY else 2 * place

    per_half = len(REACH) // 2

    def clones(g):
        for place in range(per_half):
            n = g * per_half + place
            if n:
                tag_copies[n].wait_recv()
                slot_copies[n].wait_recv()

            def one_slot(r, carry, n=n):
                marks = [
                    jnp.broadcast_to(tags[n, r, i : i + 1, :], (16, 128)).astype(jnp.bfloat16)
                    for i in range(per_device)
                ]
                for top in range(0, electrons, 16):
                    for left in range(0, basis, 128):
                        found = jnp.zeros((16, 128), jnp.bfloat16)
                        for i in range(per_device):
                            found += orb[i, top : top + 16, left : left + 128] * marks[i]
                        step = slots[n, r, top : top + 16, left : left + 128]
                        made = found.astype(jnp.float32) + step.astype(jnp.float32)
                        slots[n, r, top : top + 16, left : left + 128] = made.astype(jnp.bfloat16)
                return carry

            lax.fori_loop(0, CAP, one_slot, 0)
            wide = CAP * electrons
            turned[g, :, place * wide : (place + 1) * wide] = slots[n].reshape(wide, basis).T

    loads[2].wait()
    clones(0)
    total[...] = jnp.zeros_like(total)

    at = {}
    for when, event, of in events:
        at.setdefault(when, []).append(functools.partial(event, *of))
    for name in ORDER[1:]:
        second = range(CHUNKS) if name == "H1" else (1, 3) if name[0] == "P" else (2, 3)
        for m in second:
            at.setdefault(first_use[name], []).append(functools.partial(links.wait, (BLOCK[name], m)))
    at.setdefault(EARLY, []).append(functools.partial(clones, 1))

    e_copies = {
        n: remote(e_out.at[n], e_in.at[n], e_send.at[n], e_recv.at[n], walk_from[n]) for n in walk_ids
    }

    def energies(g):
        def energy_of(s, carry):
            n, r = s // CAP, s % CAP
            base = pl.multiple_of(s % (per_half * CAP) * electrons, electrons)
            tile = jnp.zeros((8, 128), jnp.float32)
            for top in range(0, electrons, 16):
                for left in range(0, basis, 128):
                    grad = total[g, pl.ds(base + top, 16), left : left + 128]
                    made = slots[n, r, top : top + 16, left : left + 128].astype(jnp.float32) * grad
                    tile += made[:8] + made[8:]
            e_out[n, r] = tile * -0.5
            return carry

        lax.fori_loop(g * per_half * CAP, (g + 1) * per_half * CAP, energy_of, 0)
        for n in range(g * per_half, (g + 1) * per_half):
            if n:
                e_copies[n].start()

    at.setdefault(2 * len(ORDER) - 1, []).append(functools.partial(energies, 1))

    def dispatch(t, at, first, last):
        due = [when for when in at if first <= when < last]
        if not due:
            return
        if last - first == 1:
            for event in at[first]:
                event()
            return
        middle = (first + last) // 2
        if min(due) < middle:
            pl.when(t < middle)(lambda: dispatch(t, at, first, middle))
        if max(due) >= middle:
            pl.when(t >= middle)(lambda: dispatch(t, at, middle, last))

    def half_step(t, carry):
        dispatch(t, at, 0, 2 * EARLY)
        g = jnp.where(t < EARLY, 0, 1)
        block = store.at[jnp.where(t < EARLY, t, t - EARLY)]
        meet(block, turned, inter, g)
        spread(block, inter, total, g)
        return carry

    opening = {when // 2: at[when] for when in at if when >= 2 * EARLY and when % 2 == 0}
    middle = {when // 2: at[when] for when in at if when >= 2 * EARLY and when % 2 == 1}

    def full_step(b, carry):
        dispatch(b, opening, EARLY, len(ORDER))
        block = store.at[b]
        meet(block, turned, inter, 1)
        meet(block, turned, inter, 0)
        spread(block, inter, total, 1)
        dispatch(b, middle, EARLY, len(ORDER))
        spread(block, inter, total, 0)
        return carry

    lax.fori_loop(0, 2 * EARLY, half_step, jnp.int32(0))
    lax.fori_loop(EARLY, len(ORDER), full_step, jnp.int32(0))

    energies(0)
    for n in range(len(REACH)):
        for r in range(CAP):
            for i in range(per_device):
                weights[n * CAP + r, i] = jnp.broadcast_to(-tags[n, r, i : i + 1, :], (8, 128))

    def gather(t, carry):
        top = pl.multiple_of(t // 8 * 8, 8)
        left = pl.multiple_of(t % 8 * 128, 128)
        sums = [jnp.zeros((8, 128), jnp.float32) for _ in range(per_device)]
        for s in range(len(REACH) * CAP):
            g, first = s // (per_half * CAP), s % (per_half * CAP) * electrons
            grad = total[g, pl.ds(first + top, 8), pl.ds(left, 128)]
            for i in range(per_device):
                sums[i] += weights[s, i] * grad
        for i in range(per_device):
            made_grad[i, pl.ds(top, 8), pl.ds(left, 128)] = sums[i]
        return carry

    lax.fori_loop(0, electrons * basis // 1024, gather, 0)

    store_grad = pltpu.make_async_copy(made_grad, grad_ref, load_sem.at[0])
    store_grad.start()
    for n in walk_ids:
        tag_copies[n].wait_send()
        slot_copies[n].wait_send()
    links.finish()
    for n in walk_ids:
        e_copies[n].wait()
    for j in range(per_device):
        tile = jnp.zeros((8, 128), jnp.float32)
        for n in range(len(REACH)):
            for r in range(CAP):
                used = jnp.logical_and(walker_of[n, r] == j, live_of[n, r] == 1)
                tile += jnp.where(used, 1.0, 0.0).astype(jnp.float32) * (e_in if n else e_out)[n, r]
        energy_ref[j] = tile

    store_grad.wait()


def finish(parts_ref, grad_ref, energy_ref, out_ref):
    out_ref[...] = grad_ref[...]

    @pl.when(pl.program_id(0) == 0)
    def _():
        tile = jnp.sum(parts_ref[...], axis=1)
        each = jnp.broadcast_to(jnp.sum(tile, axis=1, keepdims=True), tile.shape)
        diagonal = lax.broadcasted_iota(jnp.int32, tile.shape, 0) == lax.broadcasted_iota(jnp.int32, tile.shape, 1)
        row = jnp.sum(jnp.where(diagonal, each, 0.0), axis=0, keepdims=True)
        energy_ref[...] = row[:, : energy_ref.shape[1]]


def body(orbitals, cholesky, parents, counts, steps):
    per_device, electrons, basis = orbitals.shape
    vectors = cholesky.shape[0]
    half = NY * CAP * electrons
    reach = len(REACH)
    f32, bf16 = jnp.float32, jnp.bfloat16
    dma = pltpu.SemaphoreType.DMA
    energy, grad = pl.pallas_call(
        kernel,
        out_shape=(
            jax.ShapeDtypeStruct((per_device, 8, 128), f32),
            jax.ShapeDtypeStruct((per_device, electrons, basis), f32),
        ),
        in_specs=[pl.BlockSpec(memory_space=pltpu.SMEM)] * 2 + [pl.BlockSpec(memory_space=pl.ANY)] * 3,
        out_specs=(pl.BlockSpec(memory_space=pltpu.VMEM), pl.BlockSpec(memory_space=pl.ANY)),
        scratch_shapes=[
            pltpu.VMEM((len(ORDER), vectors, electrons, basis), bf16),
            pltpu.VMEM((per_device, electrons, basis), bf16),
            pltpu.VMEM((per_device, electrons, basis), bf16),
            pltpu.VMEM((reach, CAP, electrons, basis), bf16),
            pltpu.VMEM((reach, CAP, electrons, basis), bf16),
            pltpu.VMEM((reach, CAP, per_device, 128), f32),
            pltpu.VMEM((reach, CAP, per_device, 128), f32),
            pltpu.VMEM((2, basis, half), bf16),
            pltpu.VMEM((2, half, basis), f32),
            pltpu.VMEM((2, half, vectors * electrons), bf16),
            pltpu.VMEM((reach * CAP, per_device, 8, 128), f32),
            pltpu.VMEM((per_device, electrons, basis), f32),
            pltpu.VMEM((reach, CAP, 8, 128), f32),
            pltpu.VMEM((reach, CAP, 8, 128), f32),
            dma((3,)),
            *[dma((reach,))] * 6,
            dma((64,)),
            dma((len(ORDER) * CHUNKS,)),
        ],
        compiler_params=pltpu.CompilerParams(
            collective_id=0, has_side_effects=True, vmem_limit_bytes=60 * 2**20
        ),
        name="exchange",
    )(parents.reshape(1, -1), counts, orbitals, cholesky, steps)
    part = per_device // 2
    grad_spec = pl.BlockSpec((part, electrons, basis), lambda i: (i, 0, 0))
    energy, grad = pl.pallas_call(
        finish,
        grid=(2,),
        out_shape=(jax.ShapeDtypeStruct((1, per_device), f32), jax.ShapeDtypeStruct(grad.shape, f32)),
        in_specs=[pl.BlockSpec((per_device, 8, 128), lambda i: (0, 0, 0)), grad_spec],
        out_specs=(pl.BlockSpec((1, per_device), lambda i: (0, 0)), grad_spec),
        name="finish",
    )(energy, grad)
    return energy.reshape(per_device), grad


def solution(mesh):
    torus = Mesh(mesh.devices.reshape(NY, NH, 2, NX, 2), NAMES)
    return jax.shard_map(
        body,
        mesh=torus,
        in_specs=(
            P(NAMES, None, None),
            P(("l", "x", "k"), None, None),
            P(NAMES),
            P(("y", "h"), ("l", "x", "k")),
            P(NAMES, None, None),
        ),
        out_specs=(P(NAMES), P(NAMES, None, None)),
        check_vma=False,
    )
```
